256 devices in a mesh: slab: 8 (over x, core), rep: 32 (over z, y).
Axes of the slice: x: 4, y: 4, z: 8, core: 2. Of those that a mesh axis runs over, the one named last changes fastest.
Arguments:
- image: float32 [288, 256, 256], P('slab', 'rep'), may hold values from 0.5 to 2
- sensitivity: float32 [288, 256, 256], P('slab', 'rep'), may hold values from 0.5 to 2
- system_blocks: bfloat16 [4096, 128, 1024], P(('slab', 'rep')), may hold values from 0 to 0.00390625
- tile_slab: int32 [4096, 1], P(('slab', 'rep')), may hold values from 0 to 7; in each aligned block of 16 rows (0 to 15, 16 to 31, ...) at most 6 rows name the same one
- tile_block: int32 [4096], P(('slab', 'rep')), may hold values from 0 to 2303
- background: bfloat16 [4096, 128], P(('slab', 'rep')), may hold values from 0.19921875 to 1
Outputs:
- updated: float32 [288, 256, 256], P('slab', 'rep')
The draws below stay inside these ranges and needn't reach their ends.
Inputs may be any that keep to these rules, and one draw needn't show every extreme that they name: `tile_slab`: among the 16 tiles of one device at most 6 view the same slab, and in some devices some slab is viewed by exactly 6.
All inputs are finite; a program needn't handle non-finite values.
Results may differ from the reference program's by a relative error of at most 0.0003.
Values may be sent and summed in bfloat16 or wider, within the bound.
A program may use at most 64 MiB of HBM per device.

```python
import math
import jax
import jax.numpy as jnp
import numpy as np
from jax import lax

NX = 256
NY = 256
TILE = 128
VB = 1024
PIECES_PER_CARD = 16
CAP = 6
NZ = 288
NBLK = 2304
TILES = 4096
N_SLAB = 8


def place_ends(entries, own_key, smallest, largest):
    dims = entries.shape
    place = [jax.random.randint(jax.random.fold_in(own_key, axis), (), 0, dims[axis]) for axis in range(len(dims))]
    entries = entries.at[tuple(place)].set(smallest)
    longest = dims.index(max(dims))
    place[longest] = (place[longest] + 1) % dims[longest]
    return entries.at[tuple(place)].set(largest)


def level_of(rng, dims, pieces, low, top_value):
    def one(axis_at, blocks):
        draws = jax.random.uniform(jax.random.fold_in(jax.random.fold_in(rng, 6), axis_at), (blocks,), jnp.float32, low / len(pieces), top_value / len(pieces))
        return jnp.repeat(jnp.exp(draws), dims[axis_at] // blocks).reshape((-1,) + (1,) * (len(dims) - axis_at - 1))

    level = one(*pieces[0])
    for cut in pieces[1:]:
        level = level * one(*cut)
    return level


def assign_block(key, own, number, rows, amount, top, limit, skew):
    ranking = jax.random.permutation(key, amount)
    heavy_load, ordinary = portions_of(amount, rows * top, limit, skew, True), portions_of(amount, rows * top, limit, skew, False)
    places = jnp.arange(amount)

    def named(sizes, turn):
        used = int((sizes > 0).sum())
        fixed = max(1, used // 4)
        shifted = fixed + (places - fixed + turn * (used - fixed)) % max(1, amount - fixed)
        return jnp.zeros((amount,), jnp.int32).at[ranking[jnp.where(places < fixed, places, shifted)]].set(jnp.asarray(sizes, jnp.int32))

    sizes = jnp.where(number % 4 == 0, named(heavy_load, number // 4), named(ordinary, number - number // 4 - 1))
    mixed = jax.random.permutation(jax.random.fold_in(own, 3), amount)
    giver, sink = mixed[0:amount // 2 * 2:2], mixed[1:amount // 2 * 2:2]
    margin = jnp.minimum(sizes[giver] - 1, limit - sizes[sink]) // 2
    margin = jnp.where((giver == ranking[0]) | (sink == ranking[0]) | (sizes[sink] == 0), 0, jnp.maximum(margin, 0))
    shifted = jax.random.randint(jax.random.fold_in(own, 4), (amount // 2,), 0, 1 << 20) % (margin + 1)
    sizes = sizes.at[giver].add(-shifted).at[sink].add(shifted)
    labels = jnp.searchsorted(jnp.cumsum(sizes), jnp.arange(rows * top), side="right").astype(jnp.int32)
    listing = labels.reshape(top, rows).T
    listing = listing[jax.random.permutation(jax.random.fold_in(own, 1), rows)]
    turn = jax.random.randint(jax.random.fold_in(own, 2), (rows, 1), 0, top)
    return jnp.take_along_axis(listing, (jnp.arange(top)[None, :] + turn) % top, axis=1)


def portions_of(count, total, reach, skew, full):
    portions = [(1 << 20) // math.isqrt(standing ** skew) + 1 for standing in range(1, count + 1)]
    largest = reach if full else min(reach, max(-(-total // count), total * portions[0] // sum(portions)))
    least = 1 if total - largest >= count - 1 else 0
    given, surplus = [largest] + [least] * (count - 1), total - largest - least * (count - 1)
    while surplus > 0:
        free = [i for i in range(1, count) if given[i] < largest] or [i for i in range(1, count) if given[i] < reach]
        whole, remaining = sum([portions[i] for i in free]), surplus
        for i in free:
            more = min(reach - given[i], max(1, remaining * portions[i] // whole), surplus)
            given[i] = given[i] + more
            surplus = surplus - more
    return np.array(given)


def setup_inputs(seed: int = 0) -> dict:
    splits = jax.random.split(jax.random.key(seed), 7)
    image = jnp.clip(jnp.exp(math.log(2.0) - 1.3862944 * jax.random.uniform(splits[0], (NZ, NY, NX), jnp.float32) ** level_of(splits[0], (NZ, NY, NX), ((0, 8), (1, 32)), -0.2, 0.2)), 0.5, 2.0)
    sensitivity = jnp.clip(jnp.exp(math.log(2.0) - 1.3862944 * jax.random.uniform(splits[1], (NZ, NY, NX), jnp.float32) ** level_of(splits[1], (NZ, NY, NX), ((0, 8), (1, 32)), -0.2, 0.2)), 0.5, 2.0)
    system_blocks = jnp.clip(0.00390625 * jax.random.uniform(splits[2], (TILES, TILE, VB), jnp.float32) ** level_of(splits[2], (TILES, TILE, VB), ((0, 256),), -0.2, 0.2), 0.0, 0.00390625).astype(jnp.bfloat16)
    tile_slab_keys = jax.random.split(jax.random.fold_in(splits[3], 1), TILES // PIECES_PER_CARD)
    tile_slab_turns = jax.random.permutation(jax.random.fold_in(splits[3], 3), TILES // PIECES_PER_CARD)
    tile_slab = jax.vmap(lambda own, number: assign_block(jax.random.fold_in(splits[3], 2), own, number, PIECES_PER_CARD, N_SLAB, 1, CAP, 2))(tile_slab_keys, tile_slab_turns).reshape((TILES, 1))
    tile_block = place_ends(jax.random.randint(splits[4], (TILES,), 0, NBLK), jax.random.fold_in(splits[4], 1), 0, NBLK - 1).astype(jnp.int32)
    background = jnp.clip(jnp.exp(math.log(1.0) - 1.6133518 * jax.random.uniform(splits[5], (TILES, TILE), jnp.float32) ** level_of(splits[5], (TILES, TILE), ((0, 256),), -0.2, 0.2)), 0.19921875, 1.0).astype(jnp.bfloat16)
    return dict(image=image, sensitivity=sensitivity, system_blocks=system_blocks, tile_slab=tile_slab, tile_block=tile_block, background=background)


def reference(image, sensitivity, system_blocks, tile_slab, tile_block, background):
    tile_rows = system_blocks.shape[1]
    width = system_blocks.shape[2]
    unrolled_emission_map = image.astype(jnp.bfloat16).reshape(-1, width)
    index = (tile_slab[:, 0].astype(jnp.int32) * NBLK + tile_block.astype(jnp.int32)).astype(jnp.int32)

    def one_group(group):
        response_operator_lines, rows_index, back_ground = group
        emission_cell_entries = unrolled_emission_map[rows_index].astype(jnp.float32)
        sys_wide = response_operator_lines.astype(jnp.float32)
        forward_projection = jnp.einsum('tev,tv->te', sys_wide, emission_cell_entries, precision=lax.Precision.HIGHEST)
        inverse_permutation = (1.0 / (forward_projection + back_ground.astype(jnp.float32))).astype(jnp.bfloat16)
        inverse_permutation = lax.optimization_barrier(inverse_permutation)
        return jnp.einsum('tev,te->tv', sys_wide, inverse_permutation.astype(jnp.float32), precision=lax.Precision.HIGHEST)

    groups = (system_blocks.reshape(-1, 16, tile_rows, width), index.reshape(-1, 16), background.reshape(-1, 16, tile_rows))
    backproj = lax.map(one_group, groups).reshape(-1, width)
    partial_value = jnp.zeros(unrolled_emission_map.shape, jnp.float32).at[index].add(backproj)
    return image * partial_value.reshape(image.shape) / sensitivity
```

```python
import functools

import jax
import jax.numpy as jnp
from jax import lax
from jax.experimental import pallas as pl
from jax.experimental.pallas import tpu as pltpu
from jax.sharding import Mesh
from jax.sharding import PartitionSpec as P

SLAB = ("x", "core")
REP = ("z", "y")
ALL = ("x", "core", "z", "y")
MESH = pl.DeviceIdType.MESH
F32, BF16, I32 = jnp.float32, jnp.bfloat16, jnp.int32
VB = 1024
PER = 8
CAP = 6
ROUND = 16
SUBS = 4


def iota(shape, axis):
    return lax.broadcasted_iota(I32, shape, axis)


def log2(n):
    assert n & (n - 1) == 0
    return n.bit_length() - 1


def split3(value):
    high = value.astype(BF16)
    rest = value - high.astype(F32)
    middle = rest.astype(BF16)
    low = (rest - middle.astype(F32)).astype(BF16)
    return high, middle, low


def column_of(row, eye):
    return jnp.sum(jnp.where(eye, row, 0.0), axis=1, keepdims=True)


def row_of(column, eye):
    return jnp.sum(jnp.where(eye, column, 0.0), axis=0, keepdims=True)


def kernel(
    sizes, nloc, tiles,
    round_ref, image_ref, slab_ref, block_ref, ground_ref, system_hbm, sens_hbm,
    out_ref, most_ref,
    system, sens, left, right, chunks, ask, asked, acc, wide, fetch, got, back, came, zsend, zcame,
    sem_local, s_chunk, r_chunk, s_ask, r_ask, s_fetch, r_fetch, s_back, r_back, s_z, r_z,
):
    nx, nc, nz, ny = sizes
    plane = nx * nc * ny
    rows = plane * PER
    half = nz // 2
    sub = VB // SUBS
    x, core, z, y = (lax.axis_index(a) for a in ALL)
    me = (x * nc + core) * ny + y

    def at(q):
        return (q // (nc * ny), (q // ny) % nc, z, q % ny)

    def along(step):
        return (x, core, (z + step) % nz, y)

    load_system = pltpu.make_async_copy(system_hbm, system, sem_local.at[0])
    load_sens = pltpu.make_async_copy(sens_hbm, sens, sem_local.at[1])
    load_system.start()
    load_sens.start()

    barrier = pltpu.get_barrier_semaphore()
    for step in range(1, nz):
        pl.semaphore_signal(barrier, inc=1, device_id=along(step), device_id_type=MESH)

    def greet(k, carry):
        pl.semaphore_signal(barrier, inc=1, device_id=at((me + k) % plane), device_id_type=MESH)
        return carry

    lax.fori_loop(1, plane, greet, 0)

    left[...] = image_ref[:, :128]
    right[...] = image_ref[:, 128:]
    for a in range(8):
        side = right if a % 2 else left
        piece = side[pl.ds(a // 2, nloc, stride=4), :]
        chunks[0, :, pl.ds(a * 128, 128)] = piece.astype(BF16)

    eye = iota((tiles, tiles), 0) == iota((tiles, tiles), 1)
    per_plane = 2 * nz * ny
    block = column_of(block_ref[...].astype(F32), eye).astype(I32)
    rep = jnp.right_shift(block & (per_plane - 1), 1)
    ztile = jnp.right_shift(rep, log2(ny))
    place = jnp.right_shift(block, log2(per_plane)) * 2 + (block & 1)
    partner = slab_ref[...] * ny + (rep & (ny - 1))
    index_col = (ztile * nloc + place + 1).astype(F32)
    code_col = (partner * nz + ztile + 1).astype(F32)
    partner_col = partner.astype(F32)
    partner_row = row_of(partner_col, eye)
    before = (partner_col == partner_row) & (iota((tiles, tiles), 0) < iota((tiles, tiles), 1))
    slot_row = partner_row * PER + jnp.sum(jnp.where(before, 1.0, 0.0), axis=0, keepdims=True)
    slot_col = column_of(slot_row, eye)
    index_row = row_of(index_col, eye)
    wide_eye = iota((tiles, 128), 0) == iota((tiles, 128), 1)
    code_row = row_of(code_col, wide_eye)
    hit = iota((rows, tiles), 0).astype(F32) == slot_row
    wanted = jnp.sum(jnp.where(hit, index_row, 0.0), axis=1, keepdims=True)
    is_code = (iota((rows, 128), 0) & (PER - 1)) == CAP
    ask[...] = jnp.where(is_code, code_row, wanted)

    for q in range(plane):
        dead = pl.ds(q * PER * 8 + CAP * 8, (PER - CAP) * 8)
        wide[dead, :] = jnp.zeros(((PER - CAP) * 8, 128), F32)
        came[dead, :] = jnp.zeros(((PER - CAP) * 8, 128), F32)

    pl.semaphore_wait(barrier, plane - 1 + nz - 1)

    def pieces(direction, step):
        if step < half:
            return range(SUBS)
        return range(SUBS // 2) if direction == 0 else range(SUBS // 2, SUBS)

    def chunk_copy(direction, step, k):
        if direction == 0:
            source, target = step - 1, step
        else:
            source, target = (nz - (step - 1)) % nz, nz - step
        lanes = pl.ds(k * sub, sub)
        return pltpu.make_async_remote_copy(
            src_ref=chunks.at[source, :, lanes],
            dst_ref=chunks.at[target, :, lanes],
            send_sem=s_chunk.at[direction, step - 1, k],
            recv_sem=r_chunk.at[direction, step - 1, k],
            device_id=along(1 if direction == 0 else nz - 1),
            device_id_type=MESH,
        )

    for k in range(SUBS):
        for direction in range(2):
            if k in pieces(direction, 1):
                chunk_copy(direction, 1, k).start()

    def slab_rows(q, count):
        return pl.ds(pl.multiple_of(q * PER * 8, PER * 8), count)

    def ask_rows(q):
        return pl.ds(pl.multiple_of(q * PER, PER), PER)

    def ask_copy(q, there):
        return pltpu.make_async_remote_copy(
            src_ref=ask.at[ask_rows(q), :],
            dst_ref=asked.at[ask_rows(there), :],
            send_sem=s_ask.at[q],
            recv_sem=r_ask.at[there],
            device_id=at(q),
            device_id_type=MESH,
        )

    def fetch_copy(q, there):
        return pltpu.make_async_remote_copy(
            src_ref=fetch.at[q],
            dst_ref=got.at[there],
            send_sem=s_fetch.at[q],
            recv_sem=r_fetch.at[there],
            device_id=at(q),
            device_id_type=MESH,
        )

    def back_copy(q, there):
        return pltpu.make_async_remote_copy(
            src_ref=back.at[slab_rows(q, CAP * 8), :],
            dst_ref=came.at[slab_rows(there, CAP * 8), :],
            send_sem=s_back.at[q],
            recv_sem=r_back.at[there],
            device_id=at(q),
            device_id_type=MESH,
        )

    def each_partner(body):
        def step(k, carry):
            body((me + k) % plane)
            return carry

        lax.fori_loop(1, plane, step, 0)

    each_partner(lambda q: ask_copy(q, me).start())
    asked[ask_rows(me), :] = ask[ask_rows(me), :]

    def arrive(step):
        for k in range(SUBS):
            for direction in range(2):
                if k in pieces(direction, step):
                    chunk_copy(direction, step, k).wait_recv()
                    if step < half and k in pieces(direction, step + 1):
                        chunk_copy(direction, step + 1, k).start()

    def add_chunk(slot, first):
        base = ((z + nz - slot) % nz) * nloc + 1
        column = iota((rows, nloc), 1) + base
        pick = jnp.where(asked[:, :nloc] == column.astype(F32), 1.0, 0.0).astype(BF16)
        value = jnp.dot(pick, chunks[slot], preferred_element_type=F32)
        if first:
            acc[...] = value
        else:
            acc[...] += value

    arrive(1)
    each_partner(lambda q: ask_copy(q, q).wait_recv())
    add_chunk(0, True)
    for step in range(1, half + 1):
        if step > 1:
            arrive(step)
        add_chunk(step, False)
        if step < half:
            add_chunk(nz - step, False)

    for a in range(8):
        back[pl.ds(a, rows, stride=8), :] = acc[:, pl.ds(a * 128, 128)]

    def send_blocks(q):
        fetch[q] = back[slab_rows(q, CAP * 8), :].astype(BF16)
        fetch_copy(q, me).start()

    each_partner(send_blocks)
    got[me] = back[slab_rows(me, CAP * 8), :].astype(BF16)

    codes = asked[pl.ds(CAP, plane, stride=PER), :]
    bins = plane * nz
    count = jnp.zeros((plane, bins), F32)
    for j in range(tiles):
        match = codes[:, j : j + 1] == (iota((plane, bins), 1) + 1).astype(F32)
        count = count + jnp.where(match, 1.0, 0.0)
    most = jnp.max(jnp.sum(count, axis=0, keepdims=True), axis=1, keepdims=True)

    width = max(rows, 128)
    strips = []
    for b in range(width // 128):
        tall = min(128, rows)
        part = asked[pl.ds(b * 128, tall), :]
        live = (iota((tall, 128), 0) & (PER - 1)) < CAP
        strips.append(row_of(part, (iota((tall, 128), 0) == iota((tall, 128), 1)) & live))
    owner_row = (strips[0] if len(strips) == 1 else jnp.concatenate(strips, axis=1))[:, :rows]

    each_partner(lambda q: fetch_copy(q, q).wait_recv())

    def widen(q, carry):
        wide[slab_rows(q, CAP * 8), :] = got[q].astype(F32)
        return carry

    lax.fori_loop(0, plane, widen, 0)
    table = jnp.concatenate(
        [wide[pl.ds(a, rows, stride=8), :].astype(BF16) for a in range(8)], axis=1
    )
    mine = jnp.where(iota((tiles, rows), 1).astype(F32) == slot_col, 1.0, 0.0).astype(BF16)
    blocks = jnp.dot(mine, table, preferred_element_type=F32).astype(BF16)

    load_system.wait()
    tile_row = iota((tiles, 128), 0)
    forward = jnp.zeros((tiles, 128), F32)
    for j in range(tiles):
        value = lax.dot_general(
            blocks, system[j], (((1,), (1,)), ((), ())), preferred_element_type=F32
        )
        forward = jnp.where(tile_row == j, value, forward)
    inverse = (1.0 / (forward + ground_ref[...].astype(F32))).astype(BF16)
    wide_row = iota((tiles, VB), 0)
    result = jnp.zeros((tiles, VB), F32)
    for j in range(tiles):
        value = jnp.dot(inverse, system[j], preferred_element_type=F32)
        result = jnp.where(wide_row == j, value, result)

    eye3 = (iota((tiles, 3 * tiles), 1) & (tiles - 1)) == iota((tiles, 3 * tiles), 0)
    put = jnp.where(iota((rows, 3 * tiles), 0).astype(F32) == row_of(slot_col, eye3), 1.0, 0.0)
    parts = jnp.concatenate(split3(result), axis=0)
    acc[...] = jnp.dot(put.astype(BF16), parts, preferred_element_type=F32)
    for a in range(8):
        back[pl.ds(a, rows, stride=8), :] = acc[:, pl.ds(a * 128, 128)]
    each_partner(lambda q: back_copy(q, me).start())
    came[slab_rows(me, CAP * 8), :] = back[slab_rows(me, CAP * 8), :]

    step_col = iota((nz, rows), 0)
    zdest = jnp.where(step_col + z >= nz, step_col + z - nz, step_col + z)
    low = (zdest * nloc + 1).astype(F32)
    goes = (owner_row >= low) & (owner_row < low + nloc)
    earlier = jnp.where(iota((rows, rows), 0) < iota((rows, rows), 1), 1.0, 0.0).astype(BF16)
    goes_one = jnp.where(goes, 1.0, 0.0)
    rank = jnp.dot(goes_one.astype(BF16), earlier, preferred_element_type=F32)
    rank = rank - (round_ref[0] * ROUND).astype(F32)
    order = iota((ROUND, rows), 0).astype(F32)
    picks, places = [], []
    for step in range(nz):
        chosen = (rank[step : step + 1, :] == order) & (goes_one[step : step + 1, :] > 0.5)
        picks.append(jnp.where(chosen, 1.0, 0.0))
        places.append(jnp.where(chosen, owner_row - low[step : step + 1, :] + 1.0, 0.0))
    pick = jnp.concatenate(picks, axis=0).astype(BF16)
    where = jnp.sum(jnp.concatenate(places, axis=0), axis=1, keepdims=True)
    tagged = where + most * 128.0

    each_partner(lambda q: back_copy(q, q).wait_recv())
    value = jnp.concatenate([came[pl.ds(a, rows, stride=8), :] for a in range(8)], axis=1)
    pick3 = jnp.concatenate([pick, pick, pick], axis=1)
    packed = jnp.dot(
        pick3, jnp.concatenate(split3(value), axis=0), preferred_element_type=F32
    )
    zsend[:, :VB] = packed
    zsend[:, VB:] = jnp.broadcast_to(tagged, (nz * ROUND, 128))

    def z_copy(step):
        own = pl.ds(step * ROUND, ROUND)
        return pltpu.make_async_remote_copy(
            src_ref=zsend.at[own, :],
            dst_ref=zcame.at[own, :],
            send_sem=s_z.at[step],
            recv_sem=r_z.at[step],
            device_id=along(step),
            device_id_type=MESH,
        )

    for step in range(1, nz):
        z_copy(step).start()
    zcame[pl.ds(0, ROUND), :] = zsend[pl.ds(0, ROUND), :]
    load_sens.wait()
    for step in range(1, nz):
        z_copy(step).wait_recv()

    tags = zcame[:, VB:]
    most_all = jnp.floor(tags * (1.0 / 128.0))
    spot = tags - most_all * 128.0
    count_z = nz * ROUND
    spot_row = row_of(spot, iota((count_z, 128), 0) == iota((count_z, 128), 1))[:, :count_z]
    lands = jnp.where((iota((nloc, count_z), 0) + 1).astype(F32) == spot_row, 1.0, 0.0).astype(BF16)
    partial = jnp.dot(
        jnp.concatenate([lands, lands, lands], axis=1),
        jnp.concatenate(split3(zcame[:, :VB]), axis=0),
        preferred_element_type=F32,
    )
    for a in range(8):
        side = right if a % 2 else left
        side[pl.ds(a // 2, nloc, stride=4), :] = partial[:, a * 128 : (a + 1) * 128]
    for t, side in enumerate((left, right)):
        lanes = pl.ds(t * 128, 128)
        out_ref[:, lanes] = image_ref[:, lanes] * side[...] / sens[:, lanes]
    largest = jnp.max(jnp.max(most_all, axis=0, keepdims=True), axis=1, keepdims=True)
    most_ref[...] = jnp.broadcast_to(largest, (8, 128))

    for direction in range(2):
        for step in range(1, half + 1):
            for k in pieces(direction, step):
                chunk_copy(direction, step, k).wait_send()

    def drain(q):
        ask_copy(q, me).wait_send()
        fetch_copy(q, me).wait_send()
        back_copy(q, me).wait_send()

    each_partner(drain)
    for step in range(1, nz):
        z_copy(step).wait_send()


def update_round(sizes, number, image, slab, block, ground, system, sens):
    nx, nc, nz, ny = sizes
    plane = nx * nc * ny
    rows = plane * PER
    tiles = system.shape[0]
    lines = image.shape[0]
    nloc = lines // 4
    half = nz // 2
    dma = pltpu.SemaphoreType.DMA
    vmem = pl.BlockSpec(memory_space=pltpu.VMEM)
    return pl.pallas_call(
        functools.partial(kernel, sizes, nloc, tiles),
        out_shape=(
            jax.ShapeDtypeStruct(image.shape, F32),
            jax.ShapeDtypeStruct((8, 128), F32),
        ),
        in_specs=[
            pl.BlockSpec(memory_space=pltpu.SMEM),
            vmem, vmem, vmem, vmem,
            pl.BlockSpec(memory_space=pl.ANY),
            pl.BlockSpec(memory_space=pl.ANY),
        ],
        out_specs=(vmem, vmem),
        scratch_shapes=[
            pltpu.VMEM(system.shape, BF16),
            pltpu.VMEM(image.shape, F32),
            pltpu.VMEM((lines, 128), F32),
            pltpu.VMEM((lines, 128), F32),
            pltpu.VMEM((nz, nloc, VB), BF16),
            pltpu.VMEM((rows, 128), F32),
            pltpu.VMEM((rows, 128), F32),
            pltpu.VMEM((rows, VB), F32),
            pltpu.VMEM((rows * 8, 128), F32),
            pltpu.VMEM((plane, CAP * 8, 128), BF16),
            pltpu.VMEM((plane, CAP * 8, 128), BF16),
            pltpu.VMEM((rows * 8, 128), F32),
            pltpu.VMEM((rows * 8, 128), F32),
            pltpu.VMEM((nz * ROUND, VB + 128), F32),
            pltpu.VMEM((nz * ROUND, VB + 128), F32),
            dma((2,)),
            dma((2, half, SUBS)),
            dma((2, half, SUBS)),
            dma((plane,)), dma((plane,)),
            dma((plane,)), dma((plane,)),
            dma((plane,)), dma((plane,)),
            dma((nz,)), dma((nz,)),
        ],
        compiler_params=pltpu.CompilerParams(
            collective_id=0, has_side_effects=True, vmem_limit_bytes=48 * 1024 * 1024
        ),
        name="osem_round",
    )(number, image, slab, block, ground, system, sens)


def local(sizes, image, sensitivity, system_blocks, tile_slab, tile_block, background):
    lines = image.shape[0] * image.shape[1]
    flat = image.reshape(lines, image.shape[2])
    rest = (
        flat, tile_slab, tile_block.reshape(1, -1), background, system_blocks,
        sensitivity.reshape(flat.shape),
    )
    first, most = update_round(sizes, jnp.zeros((1,), I32), *rest)
    needed = most[0, 0].astype(I32)

    def more(total):
        def body(state):
            number, total = state
            extra, _ = update_round(sizes, jnp.full((1,), number, I32), *rest)
            return number + 1, total + extra

        return lax.while_loop(lambda s: s[0] * ROUND < needed, body, (jnp.int32(1), total))[1]

    updated = lax.cond(needed > ROUND, more, lambda total: total, first)
    return updated.reshape(image.shape)


def solution(mesh):
    finer = Mesh(mesh.devices.reshape(4, 2, 8, 4), ALL)
    return jax.shard_map(
        functools.partial(local, (4, 2, 8, 4)),
        mesh=finer,
        in_specs=(
            P(SLAB, REP, None),
            P(SLAB, REP, None),
            P(SLAB + REP, None, None),
            P(SLAB + REP, None),
            P(SLAB + REP),
            P(SLAB + REP, None),
        ),
        out_specs=P(SLAB, REP, None),
        check_vma=False,
    )
```
